32 devices in a mesh: dp: 1, ep: 32 (over x, y, z, core).
Axes of the slice: x: 2, y: 2, z: 4, core: 2. Of those that a mesh axis runs over, the one named last changes fastest.
Arguments:
- x: bfloat16 [1, 32, 256, 3584], P('dp', 'ep')
- expert: int32 [1, 32, 256, 8], P('dp', 'ep')
- slot: int32 [1, 32, 256, 8], P('dp', 'ep')
- gate: float32 [1, 32, 256, 8], P('dp', 'ep')
- w_gate: bfloat16 [64, 3584, 2048], P('ep')
- w_up: bfloat16 [64, 3584, 2048], P('ep')
- w_down: bfloat16 [64, 2048, 3584], P('ep')
- s_gate: bfloat16 [3584, 2048], replicated
- s_up: bfloat16 [3584, 2048], replicated
- s_down: bfloat16 [2048, 3584], replicated
Outputs:
- y: bfloat16 [1, 32, 256, 3584], P('dp', 'ep')
All inputs are finite; a program needn't handle non-finite values.
Results may differ from the reference program's by a relative error of at most 0.009.
Values are sent between devices in bfloat16 or wider.
A program may use at most 2 GiB of HBM per device.

```python
import jax
import jax.numpy as jnp

MEMBERS = 32
TOKENS = 256
D = 3584
FF = 2048
TOP = 8
EXPERTS = 64
SHARED_FF = 2048
SLOTS = 5 * TOKENS * TOP // (4 * EXPERTS)


def setup_inputs(seed: int = 0, part: int = 0) -> dict:
    own, k1, k2, k3, k4, k5, k6 = jax.random.split(jax.random.key(seed), 7)
    kx, ke, kl, kg = jax.random.split(jax.random.fold_in(own, part), 4)
    devices = (1, MEMBERS)
    place = jax.random.permutation(kl, jnp.arange(EXPERTS, dtype=jnp.uint32))
    slow = ((EXPERTS + (9 * place) % EXPERTS) << ((9 * place) // EXPERTS)) // EXPERTS
    wait = (jax.random.bits(ke, (*devices, TOKENS, EXPERTS), jnp.uint32) >> 10) * slow
    expert = jnp.argsort(wait, axis=-1)[..., :TOP].astype(jnp.int32)
    chosen = jax.nn.one_hot(expert, EXPERTS, dtype=jnp.int32)
    in_line = jnp.cumsum(chosen.reshape(*devices, TOKENS * TOP, EXPERTS), axis=2) - 1
    slot = jnp.sum(in_line.reshape(chosen.shape) * chosen, axis=-1)

    def one(key, rows, columns):
        return (jax.random.normal(key, (rows, columns), jnp.float32) * rows**-0.5).astype(jnp.bfloat16)

    def weights(key, rows, columns):
        return jax.lax.map(lambda k: one(k, rows, columns), jax.random.split(key, EXPERTS))

    return {
        "x": jax.random.normal(kx, (*devices, TOKENS, D), jnp.float32).astype(jnp.bfloat16),
        "expert": expert,
        "slot": slot,
        "gate": jax.nn.softmax(jax.random.normal(kg, expert.shape, jnp.float32)),
        "w_gate": weights(k1, D, FF),
        "w_up": weights(k2, D, FF),
        "w_down": weights(k3, FF, D),
        "s_gate": one(k4, D, SHARED_FF),
        "s_up": one(k5, D, SHARED_FF),
        "s_down": one(k6, SHARED_FF, D),
    }


def einsum(form, a, b):
    return jnp.einsum(form, a.astype(jnp.float32), b.astype(jnp.float32))


def for_all(x, s_gate, s_up, s_down):
    h = jax.nn.silu(einsum("...d,df->...f", x, s_gate)) * einsum("...d,df->...f", x, s_up)
    return einsum("...f,fd->...d", h.astype(jnp.bfloat16), s_down)


def reference(x, expert, slot, gate, w_gate, w_up, w_down, s_gate, s_up, s_down):
    to_expert = jax.nn.one_hot(expert, EXPERTS, dtype=jnp.bfloat16)
    to_slot = jax.nn.one_hot(slot, SLOTS, dtype=jnp.bfloat16)
    weighted = to_expert * gate[..., None].astype(jnp.bfloat16)
    dispatch = einsum("abtke,abtkc->abtec", to_expert, to_slot).astype(jnp.bfloat16)
    combine = einsum("abtke,abtkc->abtec", weighted, to_slot).astype(jnp.bfloat16)
    z = einsum("abtec,abtd->aebcd", dispatch, x).astype(jnp.bfloat16)
    h = jax.nn.silu(einsum("aebcd,edf->aebcf", z, w_gate))
    h = (h * einsum("aebcd,edf->aebcf", z, w_up)).astype(jnp.bfloat16)
    out = einsum("aebcf,efd->aebcd", h, w_down).astype(jnp.bfloat16)
    y = einsum("abtec,aebcd->abtd", combine, out)
    return (y + for_all(x, s_gate, s_up, s_down)).astype(jnp.bfloat16)
```

```python
import jax
import jax.numpy as jnp
from jax import lax
from jax.sharding import PartitionSpec as P


BF16, F32 = jnp.bfloat16, jnp.float32


def dot(a, b):
    return jnp.dot(a, b, preferred_element_type=F32)


def after(v, *earlier):
    return lax.optimization_barrier((v, *earlier))[0]


def solution(mesh):
    n = mesh.shape["ep"]

    def swap(v, mask):
        return lax.ppermute(v, "ep", [(a, a ^ mask) for a in range(n)])

    def layer(x, expert, slot, gate, w_gate, w_up, w_down, s_gate, s_up, s_down):
        x, expert, slot, gate = x[0, 0], expert[0, 0], slot[0, 0], gate[0, 0]
        tokens, width = x.shape
        top = expert.shape[1]
        per = w_gate.shape[0]
        slots = 5 * tokens * top // (4 * per * n)
        me = lax.axis_index("ep")
        column = [[c * 8 + i for i in range(8)] for c in range(n // 8)]
        place = jnp.where(slot < slots, expert * slots + slot, -1).astype(F32)
        info = jnp.stack([place, gate.astype(BF16).astype(F32)])
        info = lax.all_gather(info, "ep", axis_index_groups=column)
        here = me % 8
        far = after(x, info)
        from_z = {g: swap(far, g << 1) if g else x for g in range(4)}

        def routes(g):
            pieces = [lax.dynamic_index_in_dim(info, here ^ (2 * g + r), 0, False) for r in range(2)]
            return [p[0].astype(jnp.int32) for p in pieces], [p[1] for p in pieces]

        rows = 4 * per * 2 * slots
        row = lax.iota(jnp.int32, rows)
        c, r, e, i = row % slots, row // slots % 2, row // (2 * slots) % per, row // (2 * slots * per)
        wanted = ((me ^ (i << 3)) * per + e) * slots + c
        block = per * 2 * slots

        def pick(g, last):
            near = after(from_z[g], *last) if last else from_z[g]
            both = jnp.concatenate([near, swap(near, 1)])
            places, _ = routes(g)
            halves = []
            for q in range(2):
                hit = (r == q)[:, None] & (places[q][:, 0][None, :] == wanted[:, None])
                for j in range(1, top):
                    hit = hit | ((r == q)[:, None] & (places[q][:, j][None, :] == wanted[:, None]))
                halves.append(hit.astype(BF16))
            chosen = jnp.concatenate(halves, axis=1)
            return dot(chosen, both).astype(BF16)

        def send(z):
            cut = [z[k * block:(k + 1) * block] for k in range(4)]
            return cut[:1] + [swap(cut[k], k << 3) for k in range(1, 4)], cut[1:]

        def ffn(parts, last):
            z = jnp.stack(parts).reshape(4, per, 2 * slots, width)
            z = z.transpose(1, 0, 2, 3).reshape(per, 8 * slots, width)
            z = after(z, *last)
            h = jax.nn.silu(jnp.einsum("ebd,edf->ebf", z, w_gate, preferred_element_type=F32))
            h = (h * jnp.einsum("ebd,edf->ebf", z, w_up, preferred_element_type=F32)).astype(BF16)
            return jnp.einsum("ebf,efd->ebd", h, w_down, preferred_element_type=F32).astype(BF16)

        def cuts(out):
            out = out.reshape(per, 4, 2 * slots, width)
            return [out[:, k].reshape(block, width) for k in range(4)]

        def reply(cut):
            return cut[:1] + [swap(cut[k], k << 3) for k in range(1, 4)]

        def combine(g, back, last):
            _, gates = routes(g)
            places, _ = routes(g)
            halves = []
            for q in range(2):
                w = jnp.zeros((tokens, rows), F32)
                for j in range(top):
                    t = (places[q][:, j][:, None] == wanted[None, :]) & (r == q)[None, :]
                    w = jnp.where(t, gates[q][:, j][:, None], w)
                halves.append(w.astype(BF16))
            weigh = jnp.concatenate(halves, axis=0)
            if last:
                weigh = after(weigh, *last)
            both = dot(weigh, jnp.concatenate(back))
            own = both[:tokens] + swap(both[tokens:].astype(BF16), 1).astype(F32)
            return own if g == 0 else swap(own.astype(BF16), g << 1)

        def shared(xs):
            h = jax.nn.silu(dot(xs, s_gate)) * dot(xs, s_up)
            return dot(h.astype(BF16), s_down)

        d0, t0 = send(pick(0, []))
        total = shared(after(x, *t0))
        d1, t1 = send(pick(1, [total]))
        o0 = cuts(ffn(d0, t1))
        b0 = reply(o0)
        d3, t3 = send(pick(3, o0))
        o1 = cuts(ffn(d1, t3))
        b1 = reply(o1)
        d2, t2 = send(pick(2, o1))
        o3 = cuts(ffn(d3, t2))
        b3 = reply(o3)
        p0 = combine(0, b0, o3)
        o2 = cuts(ffn(d2, [p0]))
        b2 = reply(o2)
        p1 = combine(1, b1, o2)
        p3 = combine(3, b3, [p1])
        p2 = combine(2, b2, [p3])
        total = total + p0 + p3.astype(F32)
        total = total + p2.astype(F32) + p1.astype(F32)
        return total.astype(BF16)[None, None]

    token = P("dp", "ep", None, None)
    weight = P("ep", None, None)

    return jax.shard_map(
        layer,
        mesh=mesh,
        in_specs=(token,) * 4 + (weight,) * 3 + (P(None, None),) * 3,
        out_specs=token,
        check_vma=False,
    )
```
